128 devices in a mesh: replica: 1, data: 128 (over z, y, x, core).
Axes of the slice: x: 4, y: 4, z: 4, core: 2. Of those that a mesh axis runs over, the one named last changes fastest.
Arguments:
- x: bfloat16 [65536, 896], P(('replica', 'data'))
- adapter_id: int32 [65536], P(('replica', 'data'))
- w_gate: bfloat16 [896, 4864], replicated
- w_up: bfloat16 [896, 4864], replicated
- w_down: bfloat16 [4864, 896], replicated
- a_gate: bfloat16 [256, 896, 4], P('data')
- b_gate: bfloat16 [256, 4, 4864], P('data')
- a_up: bfloat16 [256, 896, 4], P('data')
- b_up: bfloat16 [256, 4, 4864], P('data')
- a_down: bfloat16 [256, 4864, 4], P('data')
- b_down: bfloat16 [256, 4, 896], P('data')
- hot_ids: int32 [4], replicated
- hot_a_gate: bfloat16 [4, 896, 4], replicated
- hot_b_gate: bfloat16 [4, 4, 4864], replicated
- hot_a_up: bfloat16 [4, 896, 4], replicated
- hot_b_up: bfloat16 [4, 4, 4864], replicated
- hot_a_down: bfloat16 [4, 4864, 4], replicated
- hot_b_down: bfloat16 [4, 4, 896], replicated
Outputs:
- output: bfloat16 [65536, 896], P(('replica', 'data'))
All inputs are finite; a program needn't handle non-finite values.
Results may differ from the reference program's by a relative error of at most 0.001.
Values are sent between devices in bfloat16 or wider.
A program may use at most 1 GiB of HBM per device.

```python
import jax
import jax.numpy as jnp
from jax import lax

GROUP = 128
T_LOC = 512
D = 896
F = 4864
R = 4
N_LOC = 2
HOT_K = 4
LORA_ALPHA = 32
TOK_BLOCK = 128
TOKENS = GROUP * T_LOC
ADAPTERS = GROUP * N_LOC
CAP = T_LOC // (2 * GROUP)
LORA_SCALE = LORA_ALPHA / R


def draw_hot(hot_key):
    owner_key, local_key = jax.random.split(hot_key)
    hot_owner = jax.random.permutation(owner_key, GROUP)[:HOT_K]
    hot_local = jax.random.randint(local_key, (HOT_K,), 0, N_LOC)
    return hot_owner, hot_local


def draw_ids(id_key, hot_owner, hot_local):
    shift_key, peak_key, count_key, perm_key, cold_key, pick_key = jax.random.split(id_key, 6)
    owners = jnp.arange(GROUP)
    peak_owner = jax.random.randint(peak_key, (), 0, GROUP)
    pop_shift = jnp.where(owners == peak_owner, 0, jax.random.randint(shift_key, (GROUP,), 0, 4))
    cap_upper = jnp.maximum(CAP // (2 ** pop_shift), 1)
    cap_lower = jnp.maximum(cap_upper // 2, 1)
    counts = jax.random.randint(count_key, (GROUP, GROUP), cap_lower[None, :], cap_upper[None, :] + 1)
    counts = jnp.where(owners[None, :] == peak_owner, CAP, counts)
    count_ends = jnp.cumsum(counts, axis=1)
    positions = jnp.arange(T_LOC)

    def owner_row(end_row):
        return jnp.searchsorted(end_row, positions, side='right')

    owner_seq = jax.vmap(owner_row)(count_ends)
    owner_seq = jax.random.permutation(perm_key, owner_seq, axis=1, independent=True)
    owner_safe = jnp.minimum(owner_seq, GROUP - 1)
    hot_match = hot_owner[None, :] == owners[:, None]
    has_hot = jnp.any(hot_match, axis=1).astype(jnp.int32)
    skip_local = jnp.sum(jnp.where(hot_match, hot_local[None, :], 0), axis=1) + (1 - has_hot) * N_LOC
    pick_local = jax.random.randint(cold_key, (GROUP, T_LOC), 0, N_LOC - has_hot[owner_safe])
    pick_local = pick_local + (pick_local >= skip_local[owner_safe]).astype(jnp.int32)
    cold_ids = owner_safe * N_LOC + pick_local
    hot_list = hot_owner * N_LOC + hot_local
    hot_tok = hot_list[jax.random.randint(pick_key, (GROUP, T_LOC), 0, HOT_K)]
    tok_ids = jnp.where(owner_seq == GROUP, hot_tok, cold_ids)
    return tok_ids.reshape(TOKENS).astype(jnp.int32)


def normal_weights(w_key, shape, std):
    return (jax.random.normal(w_key, shape, jnp.float32) * std).astype(jnp.bfloat16)


def adapter_set(set_key, adapter_count):
    set_keys = jax.random.split(set_key, 6)
    b_std = 0.5 / (LORA_SCALE * R ** 0.5)
    return [
        normal_weights(set_keys[0], (adapter_count, D, R), D ** -0.5),
        normal_weights(set_keys[1], (adapter_count, R, F), b_std),
        normal_weights(set_keys[2], (adapter_count, D, R), D ** -0.5),
        normal_weights(set_keys[3], (adapter_count, R, F), b_std),
        normal_weights(set_keys[4], (adapter_count, F, R), F ** -0.5),
        normal_weights(set_keys[5], (adapter_count, R, D), b_std),
    ]


def setup_inputs(seed: int = 0, part: int = 0) -> dict:
    root_key = jax.random.key(seed)
    base_keys = jax.random.split(jax.random.fold_in(root_key, 1), 3)
    route_key = jax.random.fold_in(root_key, 3)
    hot_owner, hot_local = draw_hot(jax.random.fold_in(route_key, 2))
    tok_ids = draw_ids(jax.random.fold_in(jax.random.fold_in(route_key, 1), part), hot_owner, hot_local)
    x_key = jax.random.fold_in(jax.random.fold_in(root_key, 5), part)
    store_set = adapter_set(jax.random.fold_in(root_key, 2), ADAPTERS)
    hot_set = adapter_set(jax.random.fold_in(root_key, 4), HOT_K)
    return {
        'x': jax.random.normal(x_key, (TOKENS, D), jnp.float32).astype(jnp.bfloat16),
        'adapter_id': tok_ids,
        'w_gate': normal_weights(base_keys[0], (D, F), D ** -0.5),
        'w_up': normal_weights(base_keys[1], (D, F), D ** -0.5),
        'w_down': normal_weights(base_keys[2], (F, D), F ** -0.5),
        'a_gate': store_set[0],
        'b_gate': store_set[1],
        'a_up': store_set[2],
        'b_up': store_set[3],
        'a_down': store_set[4],
        'b_down': store_set[5],
        'hot_ids': (hot_owner * N_LOC + hot_local).astype(jnp.int32),
        'hot_a_gate': hot_set[0],
        'hot_b_gate': hot_set[1],
        'hot_a_up': hot_set[2],
        'hot_b_up': hot_set[3],
        'hot_a_down': hot_set[4],
        'hot_b_down': hot_set[5],
    }


def lora_delta(tok_rows, a_rows, b_rows):
    low_rank = jnp.einsum('td,tdr->tr', tok_rows.astype(jnp.float32), a_rows.astype(jnp.float32)).astype(jnp.bfloat16)
    delta_f = jnp.einsum('tr,trf->tf', low_rank.astype(jnp.float32), b_rows.astype(jnp.float32))
    return (LORA_SCALE * delta_f).astype(jnp.bfloat16)


def reference(x, adapter_id, w_gate, w_up, w_down, a_gate, b_gate, a_up, b_up, a_down, b_down, hot_ids, hot_a_gate, hot_b_gate, hot_a_up, hot_b_up, hot_a_down, hot_b_down):
    def block_out(block_args):
        tok_rows, tok_ids = block_args
        hot_match = tok_ids[:, None] == hot_ids[None, :]
        is_hot = jnp.any(hot_match, axis=1)
        hot_slot = jnp.sum(jnp.where(hot_match, jnp.arange(HOT_K)[None, :], 0), axis=1)

        def chosen(store_set, hot_copy):
            return jnp.where(is_hot[:, None, None], hot_copy[hot_slot], store_set[tok_ids])

        gate_act = jnp.dot(tok_rows, w_gate, preferred_element_type=jnp.float32) + lora_delta(tok_rows, chosen(a_gate, hot_a_gate), chosen(b_gate, hot_b_gate)).astype(jnp.float32)
        up_act = jnp.dot(tok_rows, w_up, preferred_element_type=jnp.float32) + lora_delta(tok_rows, chosen(a_up, hot_a_up), chosen(b_up, hot_b_up)).astype(jnp.float32)
        hidden = (jax.nn.silu(gate_act) * up_act).astype(jnp.bfloat16)
        down_out = jnp.dot(hidden, w_down, preferred_element_type=jnp.float32) + lora_delta(hidden, chosen(a_down, hot_a_down), chosen(b_down, hot_b_down)).astype(jnp.float32)
        return (tok_rows.astype(jnp.float32) + down_out).astype(jnp.bfloat16)

    blocks = lax.map(block_out, (x.reshape(TOKENS // TOK_BLOCK, TOK_BLOCK, D), adapter_id.reshape(TOKENS // TOK_BLOCK, TOK_BLOCK)))
    return blocks.reshape(TOKENS, D)
```

```python
import functools

import jax
import jax.numpy as jnp
from jax import lax
from jax.experimental import pallas as pl
from jax.experimental.pallas import tpu as pltpu
from jax.sharding import PartitionSpec as P

LORA_ALPHA = 32
BF = jnp.bfloat16
F32 = jnp.float32
MESH = pl.DeviceIdType.MESH


def dot(a, b):
    return jnp.dot(a, b, preferred_element_type=F32)


def dot_nt(a, b):
    return lax.dot_general(a, b, (((1,), (1,)), ((), ())), preferred_element_type=F32)


def one_hot(mask):
    return jnp.where(mask, 1.0, 0.0).astype(BF)


def layer_kernel(
    sizes,
    hot_ids, ids, x_hbm, wg_hbm, wu_hbm, wd_hbm,
    ag_hbm, bg_hbm, au_hbm, bu_hbm, ad_hbm, bd_hbm,
    hag_hbm, hbg_hbm, hau_hbm, hbu_hbm, had_hbm, hbd_hbm,
    out_ref,
    x_ref, wg_ref, wu_ref, wd_ref,
    ag, bg, au, bu, ad, bd, hag, hbg, hau, hbu, had, hbd,
    at_hot, at_cold, bgu_hot, bgu_cold, adt_hot, adt_cold, bd_hot, bd_cold,
    put_ref, xh_ref, yh_ref, mask_hot, h_ref, xc_ref,
    send_ref, recv_ref, ysend_ref, ret_ref,
    x_sem, small_sem, gu_sem, d_sem, send_sem, recv_sem, ysend_sem, ret_sem,
):
    group, cap, scale, split = sizes
    me = lax.axis_index("data")
    tok, d_model = x_ref.shape
    d_ff = wg_ref.shape[1]
    n_local, rank = ag.shape[0], ag.shape[1]
    n_hot = hag.shape[0]
    k_hot, k_cold = n_hot * rank, n_local * rank
    cold_rows = group * cap
    hot_rows = xh_ref.shape[0]
    tile = 256
    n_tiles = d_ff // tile

    x_copy = pltpu.make_async_copy(x_hbm, x_ref, x_sem)
    x_copy.start()
    small = [
        pltpu.make_async_copy(src, dst, small_sem.at[k])
        for k, (src, dst) in enumerate(
            [(hag_hbm, hag), (hau_hbm, hau), (hbg_hbm, hbg), (hbu_hbm, hbu), (had_hbm, had), (hbd_hbm, hbd),
             (ag_hbm, ag), (au_hbm, au), (bg_hbm, bg), (bu_hbm, bu), (ad_hbm, ad), (bd_hbm, bd)])
    ]
    for copy in small:
        copy.start()

    def gu_copies(n):
        cols = pl.ds(pl.multiple_of(n * tile, tile), tile)
        return (pltpu.make_async_copy(wg_hbm.at[:, cols], wg_ref.at[:, cols], gu_sem.at[0, n]),
                pltpu.make_async_copy(wu_hbm.at[:, cols], wu_ref.at[:, cols], gu_sem.at[1, n]))

    def start_gu(n, _):
        for copy in gu_copies(n):
            copy.start()
        return 0

    lax.fori_loop(0, n_tiles, start_gu, 0)
    d_copy = pltpu.make_async_copy(wd_hbm, wd_ref, d_sem)
    d_copy.start()

    barrier = pltpu.get_barrier_semaphore()

    def greet(k, _):
        peer = lax.rem(me + k, group)
        pl.semaphore_signal(barrier, inc=1, device_id={"data": peer}, device_id_type=MESH)
        return 0

    lax.fori_loop(1, group, greet, 0)

    id_row = ids[...]
    hot_row = id_row == hot_ids[0]
    for j in range(1, n_hot):
        hot_row = jnp.logical_or(hot_row, id_row == hot_ids[j])
    owner = jnp.where(hot_row, -1, id_row // n_local)
    slot = lax.broadcasted_iota(jnp.int32, (cold_rows, tok), 0)
    owned = (slot // cap) == owner
    before = one_hot(lax.broadcasted_iota(jnp.int32, (tok, tok), 0) < lax.broadcasted_iota(jnp.int32, (tok, tok), 1))
    hot_16 = one_hot(jnp.broadcast_to(jnp.where(hot_row, 0, -1), (16, tok)) == 0)
    cold_rank = dot(one_hot(owned), before)
    hot_rank = dot(hot_16, before)[0:1, :]
    pick_cold = one_hot(jnp.logical_and(owned, cold_rank == (slot % cap).astype(F32)))
    hot_pos = jnp.where(hot_row, hot_rank, -1.0)
    pick_hot = one_hot(lax.broadcasted_iota(jnp.int32, (hot_rows, tok), 0).astype(F32) == hot_pos)

    lane_c = lax.broadcasted_iota(jnp.int32, (128, tok), 0)
    local_flag = one_hot(jnp.logical_and(lane_c < 2 * k_cold, (lane_c % k_cold) // rank == id_row % n_local))
    lane_h = lax.broadcasted_iota(jnp.int32, (2 * k_hot, tok), 0)
    which = (lane_h % k_hot) // rank
    hot_of = jnp.full((2 * k_hot, tok), hot_ids[0], jnp.int32)
    for j in range(1, n_hot):
        hot_of = jnp.where(which == j, hot_ids[j], hot_of)
    hot_flag = one_hot(hot_of == id_row)

    x_copy.wait()
    x_all = x_ref[...]
    send_ref[:, :, 0:d_model] = dot(pick_cold, x_all).astype(BF).reshape(group, cap, d_model)
    send_ref[:, :, d_model:] = dot_nt(pick_cold, local_flag).astype(BF).reshape(group, cap, 128)
    recv_ref[pl.ds(me, 1)] = send_ref[pl.ds(me, 1)]

    pl.semaphore_wait(barrier, group - 1)

    def send_x(k, _):
        peer = lax.rem(me + k, group)
        pltpu.make_async_remote_copy(
            send_ref.at[peer], recv_ref.at[me], send_sem, recv_sem,
            device_id={"data": peer}, device_id_type=MESH).start()
        return 0

    lax.fori_loop(1, group, send_x, 0)

    xh_ref[...] = dot(pick_hot, x_all).astype(BF)
    mask_hot[...] = dot_nt(pick_hot, hot_flag).astype(BF)
    put_ref[:, 0:hot_rows] = pick_hot.T
    put_ref[:, hot_rows:] = pick_cold.T

    for copy in small:
        copy.wait()
    at_hot[0:k_hot, :] = hag[...].reshape(k_hot, d_model)
    at_hot[k_hot:, :] = hau[...].reshape(k_hot, d_model)
    at_cold[0:k_cold, :] = ag[...].reshape(k_cold, d_model)
    at_cold[k_cold:, :] = au[...].reshape(k_cold, d_model)
    for ref, g, u, k in ((bgu_hot, hbg, hbu, k_hot), (bgu_cold, bg, bu, k_cold)):
        ref[...] = jnp.zeros_like(ref)
        ref[0, 0:k, :] = g[...].reshape(k, d_ff)
        ref[1, k:2 * k, :] = u[...].reshape(k, d_ff)
    adt_hot[...] = had[...].reshape(k_hot, d_ff)
    adt_cold[...] = ad[...].reshape(k_cold, d_ff)
    bd_hot[...] = hbd[...].reshape(k_hot, d_model)
    bd_cold[...] = bd[...].reshape(k_cold, d_model)

    def expand(rows, at, bgu, mask, base, first):
        low = dot_nt(rows, at[...]).astype(BF) * mask
        m = rows.shape[0]

        def step(n, _):
            cols = pl.ds(pl.multiple_of(n * tile, tile), tile)
            if first:
                for copy in gu_copies(n):
                    copy.wait()
            gate = dot(rows, wg_ref[:, cols]) + (scale * dot(low, bgu[0, :, cols])).astype(BF).astype(F32)
            up = dot(rows, wu_ref[:, cols]) + (scale * dot(low, bgu[1, :, cols])).astype(BF).astype(F32)
            h_ref[base:base + m, cols] = (jax.nn.silu(gate) * up).astype(BF)
            return 0

        lax.fori_loop(0, n_tiles, step, 0)

    def contract(rows, adt, bdm, mask, k, base):
        m = rows.shape[0]
        h = h_ref[base:base + m, :]
        low = dot_nt(h, adt[...]).astype(BF) * mask[:, 0:k]
        parts = []
        for c in range(0, d_model, tile):
            e = min(c + tile, d_model)
            y = dot(h, wd_ref[:, c:e]) + (scale * dot(low, bdm[:, c:e])).astype(BF).astype(F32)
            parts.append((rows[:, c:e].astype(F32) + y).astype(BF))
        return parts

    def hot_part(lo, hi, first):
        rows, mask = xh_ref[lo:hi, :], mask_hot[lo:hi, :]
        expand(rows, at_hot, bgu_hot, mask, lo, first)
        if first:
            d_copy.wait()
        for c, part in enumerate(contract(rows, adt_hot, bd_hot, mask, k_hot, lo)):
            yh_ref[lo:hi, c * tile:c * tile + part.shape[1]] = part

    hot_part(0, split, True)

    pltpu.make_async_remote_copy(
        send_ref.at[pl.ds(0, group - 1)], recv_ref.at[pl.ds(0, group - 1)], send_sem, recv_sem,
        device_id={"data": lax.rem(me + 1, group)}, device_id_type=MESH).wait()
    xc_ref[...] = recv_ref[:, :, 0:d_model].reshape(cold_rows, d_model)
    mask_cold = recv_ref[:, :, d_model:].reshape(cold_rows, 128)[:, 0:2 * k_cold]
    rows_c = xc_ref[...]
    expand(rows_c, at_cold, bgu_cold, mask_cold, hot_rows, False)
    for c, part in enumerate(contract(rows_c, adt_cold, bd_cold, mask_cold, k_cold, hot_rows)):
        ysend_ref[:, :, c * tile:c * tile + part.shape[1]] = part.reshape(group, cap, part.shape[1])
    ret_ref[pl.ds(me, 1)] = ysend_ref[pl.ds(me, 1)]

    def send_y(k, _):
        peer = lax.rem(me + k, group)
        pltpu.make_async_remote_copy(
            ysend_ref.at[peer], ret_ref.at[me], ysend_sem, ret_sem,
            device_id={"data": peer}, device_id_type=MESH).start()
        return 0

    lax.fori_loop(1, group, send_y, 0)

    hot_part(split, hot_rows, False)

    pltpu.make_async_remote_copy(
        ysend_ref.at[pl.ds(0, group - 1)], ret_ref.at[pl.ds(0, group - 1)], ysend_sem, ret_sem,
        device_id={"data": lax.rem(me + 1, group)}, device_id_type=MESH).wait()
    back = ret_ref[...].reshape(cold_rows, d_model)
    out_ref[...] = (dot(put_ref[:, 0:hot_rows], yh_ref[...]) + dot(put_ref[:, hot_rows:], back)).astype(BF)


def solution(mesh):
    group = mesh.shape["data"]
    token_spec = P(("replica", "data"), None)
    store_spec = P("data", None, None)
    full_mat = P(None, None)
    full_set = P(None, None, None)
    in_specs = (token_spec, P(("replica", "data")), full_mat, full_mat, full_mat) + (store_spec,) * 6 + (P(None),) + (full_set,) * 6

    def device_step(x, adapter_id, w_gate, w_up, w_down, a_gate, b_gate, a_up, b_up, a_down, b_down, hot_ids, hot_a_gate, hot_b_gate, hot_a_up, hot_b_up, hot_a_down, hot_b_down):
        tok, d_model = x.shape
        d_ff = w_gate.shape[1]
        n_local, _, rank = a_gate.shape
        n_hot = hot_ids.shape[0]
        cap = tok // (2 * group)
        cold_rows = group * cap
        hot_rows = -(-(tok - group) // 32) * 32
        split = hot_rows // 2
        k_hot, k_cold = n_hot * rank, n_local * rank
        dma = pltpu.SemaphoreType.DMA

        def sets(n):
            return [pltpu.VMEM((n, rank, d_model), BF), pltpu.VMEM((n, rank, d_ff), BF)] * 2 + [
                pltpu.VMEM((n, rank, d_ff), BF), pltpu.VMEM((n, rank, d_model), BF)]

        scratch = [
            pltpu.VMEM((tok, d_model), BF),
            pltpu.VMEM((d_model, d_ff), BF), pltpu.VMEM((d_model, d_ff), BF), pltpu.VMEM((d_ff, d_model), BF),
            *sets(n_local), *sets(n_hot),
            pltpu.VMEM((2 * k_hot, d_model), BF), pltpu.VMEM((2 * k_cold, d_model), BF),
            pltpu.VMEM((2, 2 * k_hot, d_ff), BF), pltpu.VMEM((2, 2 * k_cold, d_ff), BF),
            pltpu.VMEM((k_hot, d_ff), BF), pltpu.VMEM((k_cold, d_ff), BF),
            pltpu.VMEM((k_hot, d_model), BF), pltpu.VMEM((k_cold, d_model), BF),
            pltpu.VMEM((tok, hot_rows + cold_rows), BF),
            pltpu.VMEM((hot_rows, d_model), BF), pltpu.VMEM((hot_rows, d_model), BF),
            pltpu.VMEM((hot_rows, 2 * k_hot), BF),
            pltpu.VMEM((hot_rows + cold_rows, d_ff), BF),
            pltpu.VMEM((cold_rows, d_model), BF),
            pltpu.VMEM((group, cap, d_model + 128), BF), pltpu.VMEM((group, cap, d_model + 128), BF),
            pltpu.VMEM((group, cap, d_model), BF), pltpu.VMEM((group, cap, d_model), BF),
            dma, dma((12,)), dma((2, d_ff // 256)), dma, dma, dma, dma, dma,
        ]
        hbm = pl.BlockSpec(memory_space=pl.ANY)
        kernel = pl.pallas_call(
            functools.partial(layer_kernel, (group, cap, LORA_ALPHA / rank, split)),
            out_shape=jax.ShapeDtypeStruct((tok, d_model), BF),
            in_specs=[pl.BlockSpec(memory_space=pltpu.SMEM), pl.BlockSpec(memory_space=pltpu.VMEM)] + [hbm] * 16,
            out_specs=pl.BlockSpec(memory_space=pltpu.VMEM),
            scratch_shapes=scratch,
            compiler_params=pltpu.CompilerParams(collective_id=0, has_side_effects=True, vmem_limit_bytes=60 * 1024 * 1024),
        )

        def t(a):
            return jnp.swapaxes(a, 1, 2)

        return kernel(hot_ids, adapter_id.reshape(1, tok), x, w_gate, w_up, w_down,
                      t(a_gate), b_gate, t(a_up), b_up, t(a_down), b_down,
                      t(hot_a_gate), hot_b_gate, t(hot_a_up), hot_b_up, t(hot_a_down), hot_b_down)

    return jax.shard_map(device_step, mesh=mesh, in_specs=in_specs, out_specs=token_spec, check_vma=False)
```

```python
import functools

import jax
import jax.numpy as jnp
from jax import lax
from jax.experimental import pallas as pl
from jax.experimental.pallas import tpu as pltpu
from jax.sharding import PartitionSpec as P

LORA_ALPHA = 32
BF = jnp.bfloat16
F32 = jnp.float32
MESH = pl.DeviceIdType.MESH


def dot(a, b):
    return jnp.dot(a, b, preferred_element_type=F32)


def dot_nt(a, b):
    return lax.dot_general(a, b, (((1,), (1,)), ((), ())), preferred_element_type=F32)


def one_hot(mask):
    return jnp.where(mask, 1.0, 0.0).astype(BF)


def layer_kernel(
    sizes,
    hid_hbm, id_hbm, x_hbm, wg_hbm, wu_hbm, wd_hbm,
    ag_hbm, bg_hbm, au_hbm, bu_hbm, ad_hbm, bd_hbm,
    hag_hbm, hbg_hbm, hau_hbm, hbu_hbm, had_hbm, hbd_hbm,
    out_ref,
    hot_ids, ids, x_ref, wg_ref, wu_ref, wd_ref,
    ag, bg, au, bu, ad, bd, hag, hbg, hau, hbu, had, hbd,
    at_ref, bgu_ref, bdn_ref,
    put_ref, xh_ref, yh_ref, mask_hot, h_ref, xc_ref,
    send_ref, recv_ref, ysend_ref, ret_ref,
    id_sem, x_sem, small_sem, gu_sem, d_sem, send_sem, recv_sem, ysend_sem, ret_sem,
):
    group, cap, scale, split, half = sizes
    me = lax.axis_index("data")
    tok, d_model = x_ref.shape
    d_ff = wg_ref.shape[1]
    n_local, rank = ag.shape[0], ag.shape[1]
    n_hot = hag.shape[0]
    k_hot, k_cold = n_hot * rank, n_local * rank
    cold_rows = group * cap
    hot_rows = xh_ref.shape[0]
    tile = 256
    n_tiles = d_ff // tile

    id_copies = [pltpu.make_async_copy(id_hbm, ids, id_sem.at[0]), pltpu.make_async_copy(hid_hbm, hot_ids, id_sem.at[1])]
    for copy in id_copies:
        copy.start()
    x_copy = pltpu.make_async_copy(x_hbm, x_ref, x_sem)
    x_copy.start()
    small = [
        pltpu.make_async_copy(src, dst, small_sem.at[k])
        for k, (src, dst) in enumerate(
            [(hag_hbm, hag), (hau_hbm, hau), (hbg_hbm, hbg), (hbu_hbm, hbu), (had_hbm, had), (hbd_hbm, hbd),
             (ag_hbm, ag), (au_hbm, au), (bg_hbm, bg), (bu_hbm, bu), (ad_hbm, ad), (bd_hbm, bd)])
    ]
    for copy in small:
        copy.start()

    gu_copies = []
    for n in range(n_tiles):
        cols = slice(n * tile, (n + 1) * tile)
        gu_copies.append((pltpu.make_async_copy(wg_hbm.at[:, cols], wg_ref.at[:, cols], gu_sem.at[0, n]),
                          pltpu.make_async_copy(wu_hbm.at[:, cols], wu_ref.at[:, cols], gu_sem.at[1, n])))
    for pair in gu_copies:
        for copy in pair:
            copy.start()
    pieces = [(lo, min(lo + 5, n_tiles)) for lo in range(0, n_tiles, 5)]
    d_copy = pltpu.make_async_copy(wd_hbm, wd_ref.at[:, 0:d_model], d_sem)

    barrier = pltpu.get_barrier_semaphore()

    def others():
        for k in range(1, group):
            p = me + k
            yield jnp.where(p >= group, p - group, p)

    for peer in others():
        pl.semaphore_signal(barrier, inc=1, device_id={"data": peer}, device_id_type=MESH)
    for copy in id_copies:
        copy.wait()

    id_row = ids[...]
    hot_row = id_row == hot_ids[0]
    for j in range(1, n_hot):
        hot_row = jnp.logical_or(hot_row, id_row == hot_ids[j])
    owner = jnp.where(hot_row, -1, id_row // n_local)
    slot = lax.broadcasted_iota(jnp.int32, (cold_rows, tok), 0)
    owned = (slot // cap) == owner
    before = one_hot(lax.broadcasted_iota(jnp.int32, (tok, tok), 0) < lax.broadcasted_iota(jnp.int32, (tok, tok), 1))
    hot_16 = one_hot(jnp.broadcast_to(jnp.where(hot_row, 0, -1), (16, tok)) == 0)
    cold_rank = dot(one_hot(owned), before)
    hot_rank = dot(hot_16, before)[0:1, :]
    pick_cold = one_hot(jnp.logical_and(owned, cold_rank == (slot % cap).astype(F32)))
    hot_pos = jnp.where(hot_row, hot_rank, -1.0)
    pick_hot = one_hot(lax.broadcasted_iota(jnp.int32, (hot_rows, tok), 0).astype(F32) == hot_pos)

    lane = lax.broadcasted_iota(jnp.int32, (128, tok), 0) % half
    is_local = jnp.logical_and(lane >= k_hot, lane < k_hot + k_cold)
    local_flag = one_hot(jnp.logical_and(is_local, (lane - k_hot) // rank == id_row % n_local))
    hot_of = jnp.full((128, tok), -1, jnp.int32)
    for j in range(n_hot):
        hot_of = jnp.where(lane // rank == j, hot_ids[j], hot_of)
    hot_flag = one_hot(hot_of == id_row)

    x_copy.wait()
    x_all = x_ref[...]
    send_ref[:, :, 0:d_model] = dot(pick_cold, x_all).astype(BF).reshape(group, cap, d_model)
    send_ref[:, :, d_model:] = dot_nt(pick_cold, local_flag).astype(BF).reshape(group, cap, 128)
    recv_ref[pl.ds(me, 1)] = send_ref[pl.ds(me, 1)]

    pl.semaphore_wait(barrier, group - 1)

    for peer in others():
        pltpu.make_async_remote_copy(
            send_ref.at[peer], recv_ref.at[me], send_sem, recv_sem,
            device_id={"data": peer}, device_id_type=MESH).start()

    xh_ref[...] = dot(pick_hot, x_all).astype(BF)
    mask_hot[...] = dot_nt(pick_hot, hot_flag).astype(BF)
    put_ref[:, 0:hot_rows] = pick_hot.T
    put_ref[:, hot_rows:] = pick_cold.T

    for copy in small:
        copy.wait()
    pad = jnp.zeros((half - k_hot - k_cold, d_model), BF)

    def both(hot, local, width):
        return [hot[...].reshape(k_hot, width), local[...].reshape(k_cold, width)]

    at_ref[...] = jnp.concatenate(both(hag, ag, d_model) + [pad] + both(hau, au, d_model) + [pad], axis=0)
    pad_ff = jnp.zeros((half - k_hot - k_cold, d_ff), BF)
    none_ff = jnp.zeros((half, d_ff), BF)
    bgu_ref[0] = jnp.concatenate(both(hbg, bg, d_ff) + [pad_ff, none_ff], axis=0)
    bgu_ref[1] = jnp.concatenate([none_ff] + both(hbu, bu, d_ff) + [pad_ff], axis=0)
    bdn_ref[...] = jnp.concatenate(both(hbd, bd, d_model) + [pad], axis=0)
    wide = jnp.zeros((128 - k_hot - k_cold, d_ff), BF)
    wd_ref[:, d_model:] = jnp.concatenate(both(had, ad, d_ff) + [wide], axis=0).T

    def expand(rows, mask, base, first):
        low = dot_nt(rows, at_ref[...]).astype(BF) * mask[:, 0:2 * half]
        m = rows.shape[0]
        for n in range(n_tiles):
            cols = slice(n * tile, (n + 1) * tile)
            if first:
                for p, (lo, hi) in enumerate(pieces):
                    if lo == n:
                        for pair in gu_copies[lo:hi]:
                            for copy in pair:
                                copy.wait()
                        if p == 1:
                            d_copy.start()
            gate = dot(rows, wg_ref[:, cols]) + (scale * dot(low, bgu_ref[0, :, cols])).astype(BF).astype(F32)
            up = dot(rows, wu_ref[:, cols]) + (scale * dot(low, bgu_ref[1, :, cols])).astype(BF).astype(F32)
            h_ref[base:base + m, cols] = (jax.nn.silu(gate) * up).astype(BF)

    def contract(rows, mask, base):
        m = rows.shape[0]
        y = dot(h_ref[base:base + m, :], wd_ref[...])
        low = y[:, d_model:d_model + half].astype(BF) * mask[:, 0:half]
        y = y[:, 0:d_model] + (scale * dot(low, bdn_ref[...])).astype(BF).astype(F32)
        return (rows.astype(F32) + y).astype(BF)

    def hot_part(lo, hi, first):
        rows, mask = xh_ref[lo:hi, :], mask_hot[lo:hi, :]
        expand(rows, mask, lo, first)
        if first:
            d_copy.wait()
        yh_ref[lo:hi, :] = contract(rows, mask, lo)

    hot_part(0, split, True)

    pltpu.make_async_remote_copy(
        send_ref.at[pl.ds(0, group - 1)], recv_ref.at[pl.ds(0, group - 1)], send_sem, recv_sem,
        device_id={"data": lax.rem(me + 1, group)}, device_id_type=MESH).wait()
    xc_ref[...] = recv_ref[:, :, 0:d_model].reshape(cold_rows, d_model)
    mask_cold = recv_ref[:, :, d_model:].reshape(cold_rows, 128)
    rows_c = xc_ref[...]
    expand(rows_c, mask_cold, hot_rows, False)
    ysend_ref[...] = contract(rows_c, mask_cold, hot_rows).reshape(group, cap, d_model)
    ret_ref[pl.ds(me, 1)] = ysend_ref[pl.ds(me, 1)]

    for peer in others():
        pltpu.make_async_remote_copy(
            ysend_ref.at[peer], ret_ref.at[me], ysend_sem, ret_sem,
            device_id={"data": peer}, device_id_type=MESH).start()

    hot_part(split, hot_rows, False)

    pltpu.make_async_remote_copy(
        ysend_ref.at[pl.ds(0, group - 1)], ret_ref.at[pl.ds(0, group - 1)], ysend_sem, ret_sem,
        device_id={"data": lax.rem(me + 1, group)}, device_id_type=MESH).wait()
    back = ret_ref[...].reshape(cold_rows, d_model)
    out_ref[...] = (dot(put_ref[:, 0:hot_rows], yh_ref[...]) + dot(put_ref[:, hot_rows:], back)).astype(BF)


def solution(mesh):
    group = mesh.shape["data"]
    token_spec = P(("replica", "data"), None)
    store_spec = P("data", None, None)
    full_mat = P(None, None)
    full_set = P(None, None, None)
    in_specs = (token_spec, P(("replica", "data")), full_mat, full_mat, full_mat) + (store_spec,) * 6 + (P(None),) + (full_set,) * 6

    def device_step(x, adapter_id, w_gate, w_up, w_down, a_gate, b_gate, a_up, b_up, a_down, b_down, hot_ids, hot_a_gate, hot_b_gate, hot_a_up, hot_b_up, hot_a_down, hot_b_down):
        tok, d_model = x.shape
        d_ff = w_gate.shape[1]
        n_local, _, rank = a_gate.shape
        n_hot = hot_ids.shape[0]
        cap = tok // (2 * group)
        cold_rows = group * cap
        hot_rows = -(-(tok - group) // 32) * 32
        split = hot_rows // 2
        half = 32
        dma = pltpu.SemaphoreType.DMA

        def sets(n):
            return [pltpu.VMEM((n, rank, d_model), BF), pltpu.VMEM((n, rank, d_ff), BF)] * 2 + [
                pltpu.VMEM((n, rank, d_ff), BF), pltpu.VMEM((n, rank, d_model), BF)]

        scratch = [
            pltpu.SMEM((n_hot,), jnp.int32), pltpu.VMEM((1, tok), jnp.int32), pltpu.VMEM((tok, d_model), BF),
            pltpu.VMEM((d_model, d_ff), BF), pltpu.VMEM((d_model, d_ff), BF), pltpu.VMEM((d_ff, d_model + 128), BF),
            *sets(n_local), *sets(n_hot),
            pltpu.VMEM((2 * half, d_model), BF), pltpu.VMEM((2, 2 * half, d_ff), BF), pltpu.VMEM((half, d_model), BF),
            pltpu.VMEM((tok, hot_rows + cold_rows), BF),
            pltpu.VMEM((hot_rows, d_model), BF), pltpu.VMEM((hot_rows, d_model), BF),
            pltpu.VMEM((hot_rows, 128), BF),
            pltpu.VMEM((hot_rows + cold_rows, d_ff), BF),
            pltpu.VMEM((cold_rows, d_model), BF),
            pltpu.VMEM((group, cap, d_model + 128), BF), pltpu.VMEM((group, cap, d_model + 128), BF),
            pltpu.VMEM((group, cap, d_model), BF), pltpu.VMEM((group, cap, d_model), BF),
            dma((2,)), dma, dma((12,)), dma((2, d_ff // 256)), dma, dma, dma, dma, dma,
        ]
        hbm = pl.BlockSpec(memory_space=pl.ANY)
        kernel = pl.pallas_call(
            functools.partial(layer_kernel, (group, cap, LORA_ALPHA / rank, split, half)),
            out_shape=pltpu.VMEM((tok, d_model), BF),
            in_specs=[hbm] * 18,
            out_specs=pl.BlockSpec(memory_space=pltpu.VMEM),
            scratch_shapes=scratch,
            compiler_params=pltpu.CompilerParams(collective_id=0, has_side_effects=True, vmem_limit_bytes=60 * 1024 * 1024),
        )

        def t(a):
            return jnp.swapaxes(a, 1, 2)

        return kernel(hot_ids, adapter_id.reshape(1, tok), x, w_gate, w_up, w_down,
                      t(a_gate), b_gate, t(a_up), b_up, t(a_down), b_down,
                      t(hot_a_gate), hot_b_gate, t(hot_a_up), hot_b_up, t(hot_a_down), hot_b_down)

    return jax.shard_map(device_step, mesh=mesh, in_specs=in_specs, out_specs=token_spec, check_vma=False)
```

```python
import functools

import jax
import jax.numpy as jnp
from jax import lax
from jax.experimental import pallas as pl
from jax.experimental.pallas import tpu as pltpu
from jax.sharding import PartitionSpec as P

LORA_ALPHA = 32
BF = jnp.bfloat16
F32 = jnp.float32
MESH = pl.DeviceIdType.MESH


def dot(a, b):
    return jnp.dot(a, b, preferred_element_type=F32)


def dot_nt(a, b):
    return lax.dot_general(a, b, (((1,), (1,)), ((), ())), preferred_element_type=F32)


def one_hot(mask):
    return jnp.where(mask, 1.0, 0.0).astype(BF)


def layer_kernel(
    sizes,
    hid_hbm, id_hbm, x_hbm, wg_hbm, wu_hbm, wd_hbm,
    ag_hbm, bg_hbm, au_hbm, bu_hbm, ad_hbm, bd_hbm,
    hag_hbm, hbg_hbm, hau_hbm, hbu_hbm, had_hbm, hbd_hbm,
    out_ref,
    hot_ids, ids, x_ref, wg_ref, wu_ref, wd_ref,
    ag, bg, au, bu, ad, bd, hag, hbg, hau, hbu, had, hbd,
    at_ref, bgu_ref, bdn_ref,
    put_ref, xh_ref, yh_ref, mask_hot, h_ref, xc_ref,
    send_ref, recv_ref, ysend_ref, ret_ref,
    id_sem, x_sem, small_sem, gu_sem, d_sem, send_sem, recv_sem, ysend_sem, ret_sem,
):
    group, cap, scale, split, half = sizes
    me = lax.axis_index("data")
    tok, d_model = x_ref.shape
    d_ff = wg_ref.shape[1]
    n_local, rank = ag.shape[0], ag.shape[1]
    n_hot = hag.shape[0]
    k_hot, k_cold = n_hot * rank, n_local * rank
    cold_rows = group * cap
    hot_rows = xh_ref.shape[0]
    tile = 256
    n_tiles = d_ff // tile

    id_copies = [pltpu.make_async_copy(id_hbm, ids, id_sem.at[0]), pltpu.make_async_copy(hid_hbm, hot_ids, id_sem.at[1])]
    for copy in id_copies:
        copy.start()
    x_copy = pltpu.make_async_copy(x_hbm, x_ref, x_sem)
    x_copy.start()
    small = [
        pltpu.make_async_copy(src, dst, small_sem.at[k])
        for k, (src, dst) in enumerate(
            [(hag_hbm, hag), (hau_hbm, hau), (hbg_hbm, hbg), (hbu_hbm, hbu), (had_hbm, had), (hbd_hbm, hbd),
             (ag_hbm, ag), (au_hbm, au), (bg_hbm, bg), (bu_hbm, bu), (ad_hbm, ad), (bd_hbm, bd)])
    ]
    for copy in small:
        copy.start()

    pieces = [(lo, min(lo + 5, n_tiles)) for lo in range(0, n_tiles, 5)]
    quarter = d_model // 4

    def gu_piece(p):
        cols = slice(pieces[p][0] * tile, pieces[p][1] * tile)
        return cols, ((wg_hbm, wg_ref, gu_sem.at[0, p]), (wu_hbm, wu_ref, gu_sem.at[1, p]))

    def start_gu(p):
        if p < len(pieces):
            cols, pair = gu_piece(p)
            for r in range(4):
                rows = slice(r * quarter, (r + 1) * quarter)
                for src, dst, sem in pair:
                    pltpu.make_async_copy(src.at[rows, cols], dst.at[rows, cols], sem).start()

    def wait_gu(p):
        cols, pair = gu_piece(p)
        for src, dst, sem in pair:
            pltpu.make_async_copy(src.at[:, cols], dst.at[:, cols], sem).wait()

    def start_d():
        step = d_ff // 4
        for r in range(4):
            rows = slice(r * step, (r + 1) * step)
            pltpu.make_async_copy(wd_hbm.at[rows, :], wd_ref.at[rows, 0:d_model], d_sem).start()

    start_gu(0)

    barrier = pltpu.get_barrier_semaphore()

    def others():
        for k in range(1, group):
            p = me + k
            yield jnp.where(p >= group, p - group, p)

    for peer in others():
        pl.semaphore_signal(barrier, inc=1, device_id={"data": peer}, device_id_type=MESH)
    for copy in id_copies:
        copy.wait()
    start_gu(1)

    id_row = ids[...]
    hot_row = id_row == hot_ids[0]
    for j in range(1, n_hot):
        hot_row = jnp.logical_or(hot_row, id_row == hot_ids[j])
    owner = jnp.where(hot_row, -1, id_row // n_local)
    slot = lax.broadcasted_iota(jnp.int32, (cold_rows, tok), 0)
    owned = (slot // cap) == owner
    before = one_hot(lax.broadcasted_iota(jnp.int32, (tok, tok), 0) < lax.broadcasted_iota(jnp.int32, (tok, tok), 1))
    hot_16 = one_hot(jnp.broadcast_to(jnp.where(hot_row, 0, -1), (16, tok)) == 0)
    cold_rank = dot(one_hot(owned), before)
    hot_rank = dot(hot_16, before)[0:1, :]
    pick_cold = one_hot(jnp.logical_and(owned, cold_rank == (slot % cap).astype(F32)))
    hot_pos = jnp.where(hot_row, hot_rank, -1.0)
    pick_hot = one_hot(lax.broadcasted_iota(jnp.int32, (hot_rows, tok), 0).astype(F32) == hot_pos)

    lane = lax.broadcasted_iota(jnp.int32, (128, tok), 0) % half
    is_local = jnp.logical_and(lane >= k_hot, lane < k_hot + k_cold)
    local_flag = one_hot(jnp.logical_and(is_local, (lane - k_hot) // rank == id_row % n_local))
    hot_of = jnp.full((128, tok), -1, jnp.int32)
    for j in range(n_hot):
        hot_of = jnp.where(lane // rank == j, hot_ids[j], hot_of)
    hot_flag = one_hot(hot_of == id_row)

    x_copy.wait()
    start_gu(2)
    x_all = x_ref[...]
    send_ref[:, :, 0:d_model] = dot(pick_cold, x_all).astype(BF).reshape(group, cap, d_model)
    send_ref[:, :, d_model:] = dot_nt(pick_cold, local_flag).astype(BF).reshape(group, cap, 128)
    recv_ref[pl.ds(me, 1)] = send_ref[pl.ds(me, 1)]

    for copy in small:
        copy.wait()
    pad = jnp.zeros((half - k_hot - k_cold, d_model), BF)

    def both(hot, local, width):
        return [hot[...].reshape(k_hot, width), local[...].reshape(k_cold, width)]

    at_ref[...] = jnp.concatenate(both(hag, ag, d_model) + [pad] + both(hau, au, d_model) + [pad], axis=0)
    pad_ff = jnp.zeros((half - k_hot - k_cold, d_ff), BF)
    none_ff = jnp.zeros((half, d_ff), BF)
    bgu_ref[0] = jnp.concatenate(both(hbg, bg, d_ff) + [pad_ff, none_ff], axis=0)
    bgu_ref[1] = jnp.concatenate([none_ff] + both(hbu, bu, d_ff) + [pad_ff], axis=0)
    bdn_ref[...] = jnp.concatenate(both(hbd, bd, d_model) + [pad], axis=0)
    wide = jnp.zeros((128 - k_hot - k_cold, d_ff), BF)
    wd_ref[:, d_model:] = jnp.concatenate(both(had, ad, d_ff) + [wide], axis=0).T

    pl.semaphore_wait(barrier, group - 1)
    for p in range(3, len(pieces)):
        start_gu(p)

    for peer in others():
        pltpu.make_async_remote_copy(
            send_ref.at[peer], recv_ref.at[me], send_sem, recv_sem,
            device_id={"data": peer}, device_id_type=MESH).start()

    xh_ref[...] = dot(pick_hot, x_all).astype(BF)
    mask_hot[...] = dot_nt(pick_hot, hot_flag).astype(BF)
    put_ref[:, 0:hot_rows] = pick_hot.T
    put_ref[:, hot_rows:] = pick_cold.T

    def expand(rows, mask, base, first):
        low = dot_nt(rows, at_ref[...]).astype(BF) * mask[:, 0:2 * half]
        m = rows.shape[0]
        for n in range(n_tiles):
            cols = slice(n * tile, (n + 1) * tile)
            if first:
                for p, (lo, hi) in enumerate(pieces):
                    if lo == n:
                        wait_gu(p)
                        if p == min(1, len(pieces) - 1):
                            start_d()
            gate = dot(rows, wg_ref[:, cols]) + (scale * dot(low, bgu_ref[0, :, cols])).astype(BF).astype(F32)
            up = dot(rows, wu_ref[:, cols]) + (scale * dot(low, bgu_ref[1, :, cols])).astype(BF).astype(F32)
            h_ref[base:base + m, cols] = (jax.nn.silu(gate) * up).astype(BF)

    def contract(rows, mask, base):
        m = rows.shape[0]
        y = dot(h_ref[base:base + m, :], wd_ref[...])
        low = y[:, d_model:d_model + half].astype(BF) * mask[:, 0:half]
        y = y[:, 0:d_model] + (scale * dot(low, bdn_ref[...])).astype(BF).astype(F32)
        return (rows.astype(F32) + y).astype(BF)

    def hot_part(lo, hi, first):
        rows, mask = xh_ref[lo:hi, :], mask_hot[lo:hi, :]
        expand(rows, mask, lo, first)
        if first:
            pltpu.make_async_copy(wd_hbm, wd_ref.at[:, 0:d_model], d_sem).wait()
        yh_ref[lo:hi, :] = contract(rows, mask, lo)

    hot_part(0, split, True)

    pltpu.make_async_remote_copy(
        send_ref.at[pl.ds(0, group - 1)], recv_ref.at[pl.ds(0, group - 1)], send_sem, recv_sem,
        device_id={"data": lax.rem(me + 1, group)}, device_id_type=MESH).wait()
    xc_ref[...] = recv_ref[:, :, 0:d_model].reshape(cold_rows, d_model)
    mask_cold = recv_ref[:, :, d_model:].reshape(cold_rows, 128)
    rows_c = xc_ref[...]
    expand(rows_c, mask_cold, hot_rows, False)
    ysend_ref[...] = contract(rows_c, mask_cold, hot_rows).reshape(group, cap, d_model)
    ret_ref[pl.ds(me, 1)] = ysend_ref[pl.ds(me, 1)]

    for peer in others():
        pltpu.make_async_remote_copy(
            ysend_ref.at[peer], ret_ref.at[me], ysend_sem, ret_sem,
            device_id={"data": peer}, device_id_type=MESH).start()

    hot_part(split, hot_rows, False)
    out_ref[...] = dot(put_ref[:, 0:hot_rows], yh_ref[...]).astype(BF)

    pltpu.make_async_remote_copy(
        ysend_ref.at[pl.ds(0, group - 1)], ret_ref.at[pl.ds(0, group - 1)], ysend_sem, ret_sem,
        device_id={"data": lax.rem(me + 1, group)}, device_id_type=MESH).wait()
    back = ret_ref[...].reshape(cold_rows, d_model)
    out_ref[...] = (out_ref[...].astype(F32) + dot(put_ref[:, hot_rows:], back)).astype(BF)


def solution(mesh):
    group = mesh.shape["data"]
    token_spec = P(("replica", "data"), None)
    store_spec = P("data", None, None)
    full_mat = P(None, None)
    full_set = P(None, None, None)
    in_specs = (token_spec, P(("replica", "data")), full_mat, full_mat, full_mat) + (store_spec,) * 6 + (P(None),) + (full_set,) * 6

    def device_step(x, adapter_id, w_gate, w_up, w_down, a_gate, b_gate, a_up, b_up, a_down, b_down, hot_ids, hot_a_gate, hot_b_gate, hot_a_up, hot_b_up, hot_a_down, hot_b_down):
        tok, d_model = x.shape
        d_ff = w_gate.shape[1]
        n_local, _, rank = a_gate.shape
        n_hot = hot_ids.shape[0]
        cap = tok // (2 * group)
        cold_rows = group * cap
        hot_rows = -(-(tok - group) // 32) * 32
        split = hot_rows // 2
        half = 32
        dma = pltpu.SemaphoreType.DMA

        def sets(n):
            return [pltpu.VMEM((n, rank, d_model), BF), pltpu.VMEM((n, rank, d_ff), BF)] * 2 + [
                pltpu.VMEM((n, rank, d_ff), BF), pltpu.VMEM((n, rank, d_model), BF)]

        scratch = [
            pltpu.SMEM((n_hot,), jnp.int32), pltpu.VMEM((1, tok), jnp.int32), pltpu.VMEM((tok, d_model), BF),
            pltpu.VMEM((d_model, d_ff), BF), pltpu.VMEM((d_model, d_ff), BF), pltpu.VMEM((d_ff, d_model + 128), BF),
            *sets(n_local), *sets(n_hot),
            pltpu.VMEM((2 * half, d_model), BF), pltpu.VMEM((2, 2 * half, d_ff), BF), pltpu.VMEM((half, d_model), BF),
            pltpu.VMEM((tok, hot_rows + cold_rows), BF),
            pltpu.VMEM((hot_rows, d_model), BF), pltpu.VMEM((hot_rows, d_model), BF),
            pltpu.VMEM((hot_rows, 128), BF),
            pltpu.VMEM((hot_rows + cold_rows, d_ff), BF),
            pltpu.VMEM((cold_rows, d_model), BF),
            pltpu.VMEM((group, cap, d_model + 128), BF), pltpu.VMEM((group, cap, d_model + 128), BF),
            pltpu.VMEM((group, cap, d_model), BF), pltpu.VMEM((group, cap, d_model), BF),
            dma((2,)), dma, dma((12,)), dma((2, -(-d_ff // 1280))), dma, dma, dma, dma, dma,
        ]
        hbm = pl.BlockSpec(memory_space=pl.ANY)
        kernel = pl.pallas_call(
            functools.partial(layer_kernel, (group, cap, LORA_ALPHA / rank, split, half)),
            out_shape=pltpu.VMEM((tok, d_model), BF),
            in_specs=[hbm] * 18,
            out_specs=pl.BlockSpec(memory_space=pltpu.VMEM),
            scratch_shapes=scratch,
            compiler_params=pltpu.CompilerParams(collective_id=0, has_side_effects=True, vmem_limit_bytes=60 * 1024 * 1024),
        )

        def t(a):
            return jnp.swapaxes(a, 1, 2)

        return kernel(hot_ids, adapter_id.reshape(1, tok), x, w_gate, w_up, w_down,
                      t(a_gate), b_gate, t(a_up), b_up, t(a_down), b_down,
                      t(hot_a_gate), hot_b_gate, t(hot_a_up), hot_b_up, t(hot_a_down), hot_b_down)

    return jax.shard_map(device_step, mesh=mesh, in_specs=in_specs, out_specs=token_spec, check_vma=False)
```

```python
import functools

import jax
import jax.numpy as jnp
from jax import lax
from jax.experimental import pallas as pl
from jax.experimental.pallas import tpu as pltpu
from jax.sharding import PartitionSpec as P

LORA_ALPHA = 32
BF = jnp.bfloat16
F32 = jnp.float32
MESH = pl.DeviceIdType.MESH


def dot(a, b):
    return jnp.dot(a, b, preferred_element_type=F32)


def dot_nt(a, b):
    return lax.dot_general(a, b, (((1,), (1,)), ((), ())), preferred_element_type=F32)


def one_hot(mask):
    return jnp.where(mask, 1.0, 0.0).astype(BF)


def layer_kernel(
    sizes,
    hid_hbm, id_hbm, x_hbm, wg_hbm, wu_hbm, wd_hbm,
    ag_hbm, bg_hbm, au_hbm, bu_hbm, ad_hbm, bd_hbm,
    hag_hbm, hbg_hbm, hau_hbm, hbu_hbm, had_hbm, hbd_hbm,
    out_ref,
    hot_ids, ids, x_ref, wg_ref, wu_ref, wd_ref,
    ag, bg, au, bu, ad, bd, hag, hbg, hau, hbu, had, hbd,
    at_ref, bgu_ref, bdn_ref,
    put_ref, xh_ref, yh_ref, mask_hot, h_ref, xc_ref,
    send_ref, recv_ref, ysend_ref, ret_ref,
    id_sem, x_sem, small_sem, gu_sem, d_sem, send_sem, recv_sem, ysend_sem, ret_sem,
):
    group, cap, scale, split, half = sizes
    me = lax.axis_index("data")
    tok, d_model = x_ref.shape
    d_ff = wg_ref.shape[1]
    n_local, rank = ag.shape[0], ag.shape[1]
    n_hot = hag.shape[0]
    k_hot, k_cold = n_hot * rank, n_local * rank
    cold_rows = group * cap
    hot_rows = xh_ref.shape[0]
    tile = 256
    n_tiles = d_ff // tile

    id_copies = [pltpu.make_async_copy(id_hbm, ids, id_sem.at[0]), pltpu.make_async_copy(hid_hbm, hot_ids, id_sem.at[1])]
    for copy in id_copies:
        copy.start()
    x_copy = pltpu.make_async_copy(x_hbm, x_ref, x_sem)
    x_copy.start()
    small = [
        pltpu.make_async_copy(src, dst, small_sem.at[k])
        for k, (src, dst) in enumerate(
            [(hag_hbm, hag), (hau_hbm, hau), (hbg_hbm, hbg), (hbu_hbm, hbu), (had_hbm, had), (hbd_hbm, hbd),
             (ag_hbm, ag), (au_hbm, au), (bg_hbm, bg), (bu_hbm, bu), (ad_hbm, ad), (bd_hbm, bd)])
    ]
    for copy in small:
        copy.start()

    pieces = [(lo, min(lo + 5, n_tiles)) for lo in range(0, n_tiles, 5)]
    quarter = d_model // 4

    def gu_piece(p):
        cols = slice(pieces[p][0] * tile, pieces[p][1] * tile)
        return cols, ((wg_hbm, wg_ref, gu_sem.at[0, p]), (wu_hbm, wu_ref, gu_sem.at[1, p]))

    def start_gu(p):
        if p < len(pieces):
            cols, pair = gu_piece(p)
            for r in range(4):
                rows = slice(r * quarter, (r + 1) * quarter)
                for src, dst, sem in pair:
                    pltpu.make_async_copy(src.at[rows, cols], dst.at[rows, cols], sem).start()

    def wait_gu(p):
        cols, pair = gu_piece(p)
        for src, dst, sem in pair:
            pltpu.make_async_copy(src.at[:, cols], dst.at[:, cols], sem).wait()

    def start_d():
        step = d_ff // 4
        for r in range(4):
            rows = slice(r * step, (r + 1) * step)
            pltpu.make_async_copy(wd_hbm.at[rows, :], wd_ref.at[rows, 0:d_model], d_sem).start()

    barrier = pltpu.get_barrier_semaphore()

    def after(k):
        p = me + k
        return jnp.where(p >= group, p - group, p)

    for k in range(1, group):
        pl.semaphore_signal(barrier, inc=1, device_id={"data": after(k)}, device_id_type=MESH)
    start_gu(0)
    for copy in id_copies:
        copy.wait()
    start_gu(1)

    id_row = ids[...]
    hot_row = id_row == hot_ids[0]
    for j in range(1, n_hot):
        hot_row = jnp.logical_or(hot_row, id_row == hot_ids[j])
    owner = id_row // n_local - me
    owner = jnp.where(hot_row, -1, jnp.where(owner < 0, owner + group, owner))
    slot = lax.broadcasted_iota(jnp.int32, (cold_rows, tok), 0)
    owned = (slot // cap) == owner
    before = one_hot(lax.broadcasted_iota(jnp.int32, (tok, tok), 0) < lax.broadcasted_iota(jnp.int32, (tok, tok), 1))
    hot_16 = one_hot(jnp.broadcast_to(jnp.where(hot_row, 0, -1), (16, tok)) == 0)
    cold_rank = dot(one_hot(owned), before)
    hot_rank = dot(hot_16, before)[0:1, :]
    pick_cold = one_hot(jnp.logical_and(owned, cold_rank == (slot % cap).astype(F32)))
    hot_pos = jnp.where(hot_row, hot_rank, -1.0)
    pick_hot = one_hot(lax.broadcasted_iota(jnp.int32, (hot_rows, tok), 0).astype(F32) == hot_pos)

    lane = lax.broadcasted_iota(jnp.int32, (128, tok), 0) % half
    is_local = jnp.logical_and(lane >= k_hot, lane < k_hot + k_cold)
    local_flag = one_hot(jnp.logical_and(is_local, (lane - k_hot) // rank == id_row % n_local))
    hot_of = jnp.full((128, tok), -1, jnp.int32)
    for j in range(n_hot):
        hot_of = jnp.where(lane // rank == j, hot_ids[j], hot_of)
    hot_flag = one_hot(hot_of == id_row)

    x_copy.wait()
    for copy in small:
        copy.wait()
    start_gu(2)
    x_all = x_ref[...]
    send_ref[:, :, 0:d_model] = dot(pick_cold, x_all).astype(BF).reshape(group, cap, d_model)
    send_ref[:, :, d_model:] = dot_nt(pick_cold, local_flag).astype(BF).reshape(group, cap, 128)
    recv_ref[0:1] = send_ref[0:1]

    half_group = group // 2

    def off(stride):
        a = (me // stride) % 4
        return jnp.where(a > 2, 4 - a, a)

    far = off(2) + off(8) + off(32) >= 2

    def send_x():
        pl.semaphore_wait(barrier, group - 1)
        for k in range(1, group):
            pltpu.make_async_remote_copy(
                send_ref.at[k], recv_ref.at[k], send_sem, recv_sem.at[k // half_group],
                device_id={"data": after(k)}, device_id_type=MESH).start()

    xh_ref[...] = dot(pick_hot, x_all).astype(BF)
    mask_hot[...] = dot_nt(pick_hot, hot_flag).astype(BF)
    put_ref[:, 0:hot_rows] = pick_hot.T
    put_ref[:, hot_rows:] = pick_cold.T

    pad = jnp.zeros((half - k_hot - k_cold, d_model), BF)

    def both(hot, local, width):
        return [hot[...].reshape(k_hot, width), local[...].reshape(k_cold, width)]

    at_ref[...] = jnp.concatenate(both(hag, ag, d_model) + [pad] + both(hau, au, d_model) + [pad], axis=0)
    pad_ff = jnp.zeros((half - k_hot - k_cold, d_ff), BF)
    none_ff = jnp.zeros((half, d_ff), BF)
    bgu_ref[0] = jnp.concatenate(both(hbg, bg, d_ff) + [pad_ff, none_ff], axis=0)
    bgu_ref[1] = jnp.concatenate([none_ff] + both(hbu, bu, d_ff) + [pad_ff], axis=0)
    bdn_ref[...] = jnp.concatenate(both(hbd, bd, d_model) + [pad], axis=0)
    wide = jnp.zeros((128 - k_hot - k_cold, d_ff), BF)
    wd_ref[:, d_model:] = jnp.concatenate(both(had, ad, d_ff) + [wide], axis=0).T

    def expand(rows, mask, base, first):
        low = dot_nt(rows, at_ref[...]).astype(BF) * mask[:, 0:2 * half]
        m = rows.shape[0]
        for n in range(n_tiles):
            cols = slice(n * tile, (n + 1) * tile)
            if first:
                for p, (lo, hi) in enumerate(pieces):
                    if lo == n:
                        wait_gu(p)
                        if p == 0:
                            for q in range(3, len(pieces)):
                                start_gu(q)
                        if p == min(1, len(pieces) - 1):
                            start_d()
                            pl.when(far)(send_x)
            gate = dot(rows, wg_ref[:, cols]) + (scale * dot(low, bgu_ref[0, :, cols])).astype(BF).astype(F32)
            up = dot(rows, wu_ref[:, cols]) + (scale * dot(low, bgu_ref[1, :, cols])).astype(BF).astype(F32)
            h_ref[base:base + m, cols] = (jax.nn.silu(gate) * up).astype(BF)

    def contract(rows, mask, base):
        m = rows.shape[0]
        y = dot(h_ref[base:base + m, :], wd_ref[...])
        low = y[:, d_model:d_model + half].astype(BF) * mask[:, 0:half]
        y = y[:, 0:d_model] + (scale * dot(low, bdn_ref[...])).astype(BF).astype(F32)
        return (rows.astype(F32) + y).astype(BF)

    def hot_part(lo, hi, first):
        rows, mask = xh_ref[lo:hi, :], mask_hot[lo:hi, :]
        expand(rows, mask, lo, first)
        if first:
            pltpu.make_async_copy(wd_hbm, wd_ref.at[:, 0:d_model], d_sem).wait()
            pl.when(jnp.logical_not(far))(send_x)
        yh_ref[lo:hi, :] = contract(rows, mask, lo)

    hot_part(0, split, True)

    half_rows = half_group * cap
    for part in range(2):
        lo, hi = part * half_group, (part + 1) * half_group
        first = max(lo, 1)
        pltpu.make_async_remote_copy(
            send_ref.at[pl.ds(first, hi - first)], recv_ref.at[pl.ds(first, hi - first)], send_sem, recv_sem.at[part],
            device_id={"data": after(1)}, device_id_type=MESH).wait_recv()
        base = part * half_rows
        xc_ref[base:base + half_rows, :] = recv_ref[lo:hi, :, 0:d_model].reshape(half_rows, d_model)
        mask_cold = recv_ref[lo:hi, :, d_model:].reshape(half_rows, 128)
        rows_c = xc_ref[base:base + half_rows, :]
        expand(rows_c, mask_cold, hot_rows + base, False)
        ysend_ref[lo:hi] = contract(rows_c, mask_cold, hot_rows + base).reshape(half_group, cap, d_model)
        if part == 0:
            ret_ref[0:1] = ysend_ref[0:1]
        for k in range(first, hi):
            pltpu.make_async_remote_copy(
                ysend_ref.at[k], ret_ref.at[k], ysend_sem, ret_sem,
                device_id={"data": after(group - k)}, device_id_type=MESH).start()

    hot_part(split, hot_rows, False)
    out_ref[...] = dot(put_ref[:, 0:hot_rows], yh_ref[...]).astype(BF)

    pltpu.make_async_remote_copy(
        send_ref.at[pl.ds(1, group - 1)], recv_ref.at[pl.ds(1, group - 1)], send_sem, recv_sem.at[0],
        device_id={"data": after(1)}, device_id_type=MESH).wait_send()
    pltpu.make_async_remote_copy(
        ysend_ref.at[pl.ds(1, group - 1)], ret_ref.at[pl.ds(1, group - 1)], ysend_sem, ret_sem,
        device_id={"data": after(1)}, device_id_type=MESH).wait()
    back = ret_ref[...].reshape(cold_rows, d_model)
    out_ref[...] = (out_ref[...].astype(F32) + dot(put_ref[:, hot_rows:], back)).astype(BF)


def solution(mesh):
    group = mesh.shape["data"]
    token_spec = P(("replica", "data"), None)
    store_spec = P("data", None, None)
    full_mat = P(None, None)
    full_set = P(None, None, None)
    in_specs = (token_spec, P(("replica", "data")), full_mat, full_mat, full_mat) + (store_spec,) * 6 + (P(None),) + (full_set,) * 6

    def device_step(x, adapter_id, w_gate, w_up, w_down, a_gate, b_gate, a_up, b_up, a_down, b_down, hot_ids, hot_a_gate, hot_b_gate, hot_a_up, hot_b_up, hot_a_down, hot_b_down):
        tok, d_model = x.shape
        d_ff = w_gate.shape[1]
        n_local, _, rank = a_gate.shape
        n_hot = hot_ids.shape[0]
        cap = tok // (2 * group)
        cold_rows = group * cap
        hot_rows = -(-(tok - group) // 32) * 32
        split = hot_rows // 2
        half = 32
        dma = pltpu.SemaphoreType.DMA

        def sets(n):
            return [pltpu.VMEM((n, rank, d_model), BF), pltpu.VMEM((n, rank, d_ff), BF)] * 2 + [
                pltpu.VMEM((n, rank, d_ff), BF), pltpu.VMEM((n, rank, d_model), BF)]

        scratch = [
            pltpu.SMEM((n_hot,), jnp.int32), pltpu.VMEM((1, tok), jnp.int32), pltpu.VMEM((tok, d_model), BF),
            pltpu.VMEM((d_model, d_ff), BF), pltpu.VMEM((d_model, d_ff), BF), pltpu.VMEM((d_ff, d_model + 128), BF),
            *sets(n_local), *sets(n_hot),
            pltpu.VMEM((2 * half, d_model), BF), pltpu.VMEM((2, 2 * half, d_ff), BF), pltpu.VMEM((half, d_model), BF),
            pltpu.VMEM((tok, hot_rows + cold_rows), BF),
            pltpu.VMEM((hot_rows, d_model), BF), pltpu.VMEM((hot_rows, d_model), BF),
            pltpu.VMEM((hot_rows, 128), BF),
            pltpu.VMEM((hot_rows + cold_rows, d_ff), BF),
            pltpu.VMEM((cold_rows, d_model), BF),
            pltpu.VMEM((group, cap, d_model + 128), BF), pltpu.VMEM((group, cap, d_model + 128), BF),
            pltpu.VMEM((group, cap, d_model), BF), pltpu.VMEM((group, cap, d_model), BF),
            dma((2,)), dma, dma((12,)), dma((2, -(-d_ff // 1280))), dma, dma, dma((2,)), dma, dma,
        ]
        hbm = pl.BlockSpec(memory_space=pl.ANY)
        kernel = pl.pallas_call(
            functools.partial(layer_kernel, (group, cap, LORA_ALPHA / rank, split, half)),
            out_shape=pltpu.VMEM((tok, d_model), BF),
            in_specs=[hbm] * 18,
            out_specs=pl.BlockSpec(memory_space=pltpu.VMEM),
            scratch_shapes=scratch,
            compiler_params=pltpu.CompilerParams(collective_id=0, has_side_effects=True, vmem_limit_bytes=60 * 1024 * 1024),
        )

        def t(a):
            return jnp.swapaxes(a, 1, 2)

        return kernel(hot_ids, adapter_id.reshape(1, tok), x, w_gate, w_up, w_down,
                      t(a_gate), b_gate, t(a_up), b_up, t(a_down), b_down,
                      t(hot_a_gate), hot_b_gate, t(hot_a_up), hot_b_up, t(hot_a_down), hot_b_down)

    return jax.shard_map(device_step, mesh=mesh, in_specs=in_specs, out_specs=token_spec, check_vma=False)
```
